32 devices in a mesh: rep: 2 (over x), dp: 16 (over y, z, core).
Axes of the slice: x: 2, y: 2, z: 4, core: 2. Of those that a mesh axis runs over, the one named last changes fastest.
Arguments:
- g_w_gate: bfloat16 [32, 2, 1024, 3200], P(('rep', 'dp')), parts along dimension 0
- g_w_up: bfloat16 [32, 2, 1024, 3200], P(('rep', 'dp')), parts along dimension 0
- g_w_down: bfloat16 [32, 2, 3200, 1024], P(('rep', 'dp')), parts along dimension 0
- w_gate: bfloat16 [2, 1024, 3200], replicated
- w_up: bfloat16 [2, 1024, 3200], replicated
- w_down: bfloat16 [2, 3200, 1024], replicated
- m_w_gate: float32 [2, 1024, 3200], P(None, 'dp')
- m_w_up: float32 [2, 1024, 3200], P(None, 'dp')
- m_w_down: float32 [2, 3200, 1024], P(None, 'dp')
- v_w_gate: float32 [2, 1024, 3200], P(None, 'dp')
- v_w_up: float32 [2, 1024, 3200], P(None, 'dp')
- v_w_down: float32 [2, 3200, 1024], P(None, 'dp')
Outputs:
- output 1: bfloat16 [4, 1024, 3200], P('rep'), parts along dimension 0
- output 2: bfloat16 [4, 1024, 3200], P('rep'), parts along dimension 0
- output 3: bfloat16 [4, 3200, 1024], P('rep'), parts along dimension 0
- output 4: float32 [4, 1024, 3200], P('rep', 'dp'), parts along dimension 0
- output 5: float32 [4, 1024, 3200], P('rep', 'dp'), parts along dimension 0
- output 6: float32 [4, 3200, 1024], P('rep', 'dp'), parts along dimension 0
- output 7: float32 [4, 1024, 3200], P('rep', 'dp'), parts along dimension 0
- output 8: float32 [4, 1024, 3200], P('rep', 'dp'), parts along dimension 0
- output 9: float32 [4, 3200, 1024], P('rep', 'dp'), parts along dimension 0
There are 2 independent parts. The reference program is written for one: setup_inputs(seed, part) draws one part's arguments, and reference() takes and returns one part's arrays. A program takes and returns all parts, laid end to end along the dimension named above; an argument that names none is the same for every part.
All inputs are finite; a program needn't handle non-finite values.
Results may differ from the reference program's by a relative error of at most 0.022.
Values are sent between devices in bfloat16 or wider.
A program may use at most 2 GiB of HBM per device.

```python
import jax
import jax.numpy as jnp
from jax import lax

DEVICES = 16
D = 1024
FF = 3200
LAYERS = 2
NAMES = ("w_gate", "w_up", "w_down")
SHAPES = {"w_gate": (LAYERS, D, FF), "w_up": (LAYERS, D, FF), "w_down": (LAYERS, FF, D)}


def setup_inputs(seed: int = 0, part: int = 0) -> dict:
    kz, *keys = jax.random.split(jax.random.key(seed), 1 + 5 * len(NAMES))
    loud = 2.0 ** jax.random.uniform(kz, (), jnp.float32, -1.0, 1.0)
    drawn = {}
    for name, key, both in zip(NAMES, keys[:3], keys[3:6], strict=True):
        own = jax.random.normal(jax.random.fold_in(key, part), (DEVICES, *SHAPES[name]), jnp.float32)
        shared = jax.random.normal(jax.random.fold_in(both, part), SHAPES[name], jnp.float32)
        drawn["g_" + name] = (loud * (0.7 * shared / DEVICES + 0.7 * own * DEVICES**-0.5)).astype(jnp.bfloat16)
    for name, key in zip(NAMES, keys[6:9], strict=True):
        drawn[name] = (jax.random.normal(key, SHAPES[name], jnp.float32) * SHAPES[name][1] ** -0.5).astype(jnp.bfloat16)
    for name, key in zip(NAMES, keys[9:12], strict=True):
        drawn["m_" + name] = loud * 0.5 * jax.random.normal(key, SHAPES[name], jnp.float32)
    for name, key in zip(NAMES, keys[12:15], strict=True):
        drawn["v_" + name] = loud * loud * jax.random.uniform(key, SHAPES[name], jnp.float32, 0.5, 1.5)
    return drawn


def adamw(w, m, v, g):
    m = 0.9 * m + 0.1 * g
    v = 0.95 * v + 0.05 * g * g
    step = m * lax.rsqrt(v + 1e-8) + 0.1 * w
    return (w - 0.02 * step).astype(jnp.bfloat16), m, v


def reference(g_w_gate, g_w_up, g_w_down, w_gate, w_up, w_down, m_w_gate, m_w_up, m_w_down, v_w_gate, v_w_up, v_w_down):
    def total(terms):
        return lax.scan(lambda so_far, term: (so_far + term.astype(jnp.float32), None), jnp.zeros(terms.shape[1:], jnp.float32), terms)[0]

    gradients = [total(terms).astype(jnp.bfloat16).astype(jnp.float32) for terms in (g_w_gate, g_w_up, g_w_down)]
    new = [
        adamw(w.astype(jnp.float32), m, v, g)
        for w, m, v, g in zip((w_gate, w_up, w_down), (m_w_gate, m_w_up, m_w_down), (v_w_gate, v_w_up, v_w_down), gradients, strict=True)
    ]
    return tuple(one[which] for which in range(3) for one in new)
```

```python
import functools

import jax
import jax.numpy as jnp
from jax import lax
from jax.experimental import pallas as pl
from jax.experimental.pallas import tpu as pltpu
from jax.sharding import PartitionSpec as P

PIECES = 10
RING = 8
LAG = 4
F32, BF16 = jnp.float32, jnp.bfloat16


def kernel(pieces, tiles, near, refs_in, refs_out, scratch):
    g_in, w_in, m_in, v_in = (refs_in[i : i + 3] for i in (0, 3, 6, 9))
    out, m_out, v_out = refs_out
    (G, CL, A1, AL, AR, BL, BR, B2, NW, W, M, V, GS) = scratch[:13]
    (l_g, l_mv, l_st, l_out) = scratch[13:17]
    (r_core, r_a1, r_al, r_ar, r_bl, r_br, r_b2, r_yo, r_az, r_ay, r_bz, r_co) = scratch[17:29]
    (s_core, s_a1, s_al, s_ar, s_bl, s_br, s_b2, s_yo, s_azr, s_azl, s_ay, s_bzr, s_bzl, s_co) = scratch[29:]
    T = tiles // pieces
    TA, TB = near, T - near
    N = 6 * pieces
    x, me = lax.axis_index("rep"), lax.axis_index("dp")
    core, z, y = me % 2, (me // 2) % 4, me // 8
    partner, right, left, across = me + 1 - 2 * core, me + 2, me - 2, me + 8 - 16 * y

    barrier = pltpu.get_barrier_semaphore()

    def greet(device):
        pl.semaphore_signal(barrier, inc=1, device_id=(x, device), device_id_type=pl.DeviceIdType.MESH)

    greet(partner)
    greet(across)

    @pl.when(z > 0)
    def _():
        greet(left)

    @pl.when(z < 3)
    def _():
        greet(right)

    pl.semaphore_wait(barrier, 2 + jnp.where(z > 0, 1, 0) + jnp.where(z < 3, 1, 0))

    def copy(src, dst, ss, rs, device):
        return pltpu.make_async_remote_copy(
            src_ref=src, dst_ref=dst, send_sem=ss, recv_sem=rs, device_id=(x, device), device_id_type=pl.DeviceIdType.MESH
        )

    def place(c):
        w = c // (2 * pieces)
        r = c - w * 2 * pieces
        layer = r // pieces
        return w, layer, (r - layer * pieces) * T

    both, row, near_part, far_part = pl.ds(0, 2), pl.ds(0, 4), pl.ds(0, TA), pl.ds(TA, TB)

    def c_core(c, i):
        _, layer, at = place(c)
        src = g_in[i].at[layer, both, row, 1 - core, pl.ds(at, T)]
        return copy(src, CL.at[c], s_core.at[c % RING], r_core.at[c], partner)

    def c_g(c, i):
        _, layer, at = place(c)
        return pltpu.make_async_copy(g_in[i].at[layer, both, row, core, pl.ds(at, T)], G.at[c % RING], l_g.at[c % RING])

    def c_load(c, i):
        _, layer, at = place(c)
        k = c % 4
        return (
            pltpu.make_async_copy(m_in[i].at[layer, pl.ds(at, T)], M.at[k], l_mv.at[k, 0]),
            pltpu.make_async_copy(v_in[i].at[layer, pl.ds(at, T)], V.at[k], l_mv.at[k, 1]),
            pltpu.make_async_copy(w_in[i].at[layer, y, z, core, pl.ds(at, T)], W.at[k], l_mv.at[k, 2]),
        )

    def c_store(c):
        w, layer, at = place(c)
        k = c % 4
        return (
            pltpu.make_async_copy(M.at[k], m_out.at[w, layer, pl.ds(at, T)], l_st.at[k, 0]),
            pltpu.make_async_copy(V.at[k], v_out.at[w, layer, pl.ds(at, T)], l_st.at[k, 1]),
        )

    def c_a1(c):
        return copy(CL.at[c, 1 - y, row, near_part], A1.at[c], s_a1.at[c % RING], r_a1.at[c], across)

    def c_a2(c, b, go_right):
        land, rs, ss, k, device = (AL, r_al, s_al, b - 1, right) if go_right else (AR, r_ar, s_ar, b, left)
        return copy(CL.at[c, y, b, near_part], land.at[c, k], ss.at[c % RING, k], rs.at[c, k], device)

    def c_b1(c, b, go_right):
        land, rs, ss, k, device = (BL, r_bl, s_bl, b - 1, right) if go_right else (BR, r_br, s_br, b, left)
        return copy(CL.at[c, both, b, far_part], land.at[c, k], ss.at[c % RING, k], rs.at[c, k], device)

    def c_b2(c):
        return copy(CL.at[c, 1 - y, z, far_part], B2.at[c], s_b2.at[c % RING], r_b2.at[c], across)

    def spot(c, rows, column, at, n):
        w, layer, start = place(c)
        return out.at[w, layer, rows, column, core, pl.ds(start + at, n)]

    def c_own(c):
        return pltpu.make_async_copy(NW.at[c % RING], spot(c, y, z, 0, T), l_out.at[c % RING])

    def c_yo(c):
        return copy(NW.at[c % RING], spot(c, y, z, 0, T), s_yo.at[c % RING], r_yo.at[c], across)

    def c_az(c, b, go_right, own=False):
        ss, device = (s_azr, right) if go_right else (s_azl, left)
        src = NW.at[c % RING, near_part] if own else spot(c, y, b, 0, TA)
        return copy(src, spot(c, y, b, 0, TA), ss.at[c % RING, b], r_az.at[c, b], device)

    def c_ay(c, b):
        return copy(spot(c, y, b, 0, TA), spot(c, y, b, 0, TA), s_ay.at[c % RING, b], r_ay.at[c, b], across)

    def c_bz(c, b, go_right):
        ss, device = (s_bzr, right) if go_right else (s_bzl, left)
        return copy(spot(c, both, b, TA, TB), spot(c, both, b, TA, TB), ss.at[c % RING, b], r_bz.at[c, b], device)

    def c_co(c, b):
        return copy(spot(c, both, b, 0, T), spot(c, both, b, 0, T), s_co.at[c % RING, b], r_co.at[c, b], partner)

    def start(copies):
        for one in copies if isinstance(copies, tuple) else (copies,):
            one.start()

    def sent(one):
        one.wait_send()

    def ok(c):
        return jnp.logical_and(c >= 0, c < N)

    def when(*conds):
        return pl.when(functools.reduce(jnp.logical_and, conds))

    def loop(low, high, body):
        lax.fori_loop(low, high, lambda i, _: (body(i), 0)[1], 0)

    def of_weight(c, do):
        w = c // (2 * pieces)
        for i in range(3):

            @pl.when(w == i)
            def _():
                do(i)

    def total(terms):
        return functools.reduce(jnp.add, (one.astype(F32) for one in terms))

    def a2(c, go_right, act, sums):
        def one(b):
            if sums:

                def put(inner):
                    terms = [G[c % RING, y, b, near_part], CL[c, y, b, near_part], A1[c, b]]
                    if inner:
                        terms.append(AL[c, b - 1] if go_right else AR[c, b])
                    CL[c, y, b, near_part] = total(terms).astype(BF16)

                pl.when(z == (0 if go_right else 3))(lambda: put(False))
                pl.when(z != (0 if go_right else 3))(lambda: put(True))
            act(c_a2(c, b, go_right))

        loop(z + 1, 4, one) if go_right else loop(0, z, one)

    def b1(c, go_right, act, sums):
        def one(b):
            if sums:

                def put(inner):
                    terms = [G[c % RING, both, b, far_part], CL[c, both, b, far_part]]
                    if inner:
                        terms.append(BL[c, b - 1] if go_right else BR[c, b])
                    CL[c, both, b, far_part] = total(terms).astype(BF16)

                pl.when(z == (0 if go_right else 3))(lambda: put(False))
                pl.when(z != (0 if go_right else 3))(lambda: put(True))
            act(c_b1(c, b, go_right))

        loop(z + 1, 4, one) if go_right else loop(0, z, one)

    def arrived(c, go_right, make):
        if go_right:
            when(z > 0)(lambda: loop(z, 4, lambda b: make(c, b, True).wait_recv()))
        else:
            when(z < 3)(lambda: loop(0, z + 1, lambda b: make(c, b, False).wait_recv()))

    def own_part(c, yy, part, with_rows, land_l, land_r, extra, put):
        def terms():
            return [G[c % RING, yy, z, part], CL[c, yy, z, part], *extra()]

        def from_left():
            return land_l[c, z - 1, yy] if with_rows else land_l[c, z - 1]

        def from_right():
            return land_r[c, z, yy] if with_rows else land_r[c, z]

        pl.when(z == 0)(lambda: put(total([*terms(), from_right()])))
        pl.when(z == 3)(lambda: put(total([*terms(), from_left()])))
        when(z > 0, z < 3)(lambda: put(total([*terms(), from_left(), from_right()])))

    def az(c, b, act, own=False):
        when(z < 3, b <= z)(lambda: act(c_az(c, b, True, own)))
        when(z > 0, b >= z)(lambda: act(c_az(c, b, False, own)))

    def bz(c, b, act):
        when(z < 3, b <= z)(lambda: act(c_bz(c, b, True)))
        when(z > 0, b >= z)(lambda: act(c_bz(c, b, False)))

    def step(t):
        @pl.when(t < N)
        def _():
            of_weight(t, lambda i: (start(c_core(t, i)), start(c_g(t, i))))

        c0 = t - 4

        @when(ok(c0))
        def _():
            @pl.when(c0 >= 4)
            def _():
                for one in c_store(c0 - 4):
                    one.wait()

            of_weight(c0, lambda i: start(c_load(c0, i)))

        tau = t - 2

        @when(ok(tau))
        def _():
            c_g(tau, 0).wait()
            c_core(tau, 0).wait_recv()

            def add(b):
                CL[tau, 1 - y, b, near_part] = total((G[tau % RING, 1 - y, b, near_part], CL[tau, 1 - y, b, near_part])).astype(BF16)

            loop(0, 4, add)
            c_a1(tau).start()

        for go_right in (True, False):
            c = tau - z if go_right else tau - 3 + z

            @when(ok(c))
            def _():
                arrived(c, go_right, c_b1)
                b1(c, go_right, start, True)

        @when(ok(tau - 1))
        def _():
            c_a1(tau - 1).wait_recv()

        for go_right in (True, False):
            c = tau - 1 - z if go_right else tau - 4 + z

            @when(ok(c))
            def _():
                arrived(c, go_right, c_a2)
                a2(c, go_right, start, True)

        c3 = tau - 3

        @when(ok(c3))
        def _():
            def put(value):
                CL[c3, 1 - y, z, far_part] = value.astype(BF16)

            own_part(c3, 1 - y, far_part, True, BL, BR, lambda: (), put)
            c_b2(c3).start()

        c4 = tau - 4

        @when(ok(c4))
        def _():
            c_b2(c4).wait_recv()
            for one in c_load(c4, 0):
                one.wait()

            def put_near(value):
                GS[near_part] = value.astype(BF16)

            def put_far(value):
                GS[far_part] = value.astype(BF16)

            own_part(c4, y, near_part, False, AL, AR, lambda: (A1[c4, z],), put_near)
            own_part(c4, y, far_part, True, BL, BR, lambda: (B2[c4],), put_far)
            k = c4 % 4
            g = GS[...].astype(F32)
            m = 0.9 * M[k] + 0.1 * g
            v = 0.95 * V[k] + 0.05 * g * g
            w = W[k].astype(F32)
            NW[c4 % RING] = (w - 0.02 * (m * lax.rsqrt(v + 1e-8) + 0.1 * w)).astype(BF16)
            M[k] = m
            V[k] = v
            c_yo(c4).start()
            az(c4, z, start, True)
            c_own(c4).start()
            start(c_store(c4))

        for k in (1, 2, 3):
            c = tau - 4 - k
            for b, there in ((z - k, z - k >= 0), (z + k, z + k <= 3)):

                @when(ok(c), there)
                def _():
                    c_az(c, b, True).wait_recv()
                    az(c, b, start)
                    c_ay(c, b).start()

        for k in (0, 1, 2, 3):
            c = tau - 5 - k
            for b, there in ((z - k, z - k >= 0), (z + k, z + k <= 3))[: 1 if k == 0 else 2]:

                @when(ok(c), there)
                def _():
                    if k == 0:
                        c_yo(c).wait_recv()
                        c_own(c).wait()
                    else:
                        c_bz(c, b, True).wait_recv()
                        c_ay(c, b).wait_recv()
                    bz(c, b, start)
                    c_co(c, b).start()

        c10 = tau - 10

        @when(ok(c10))
        def _():
            loop(0, 4, lambda b: c_co(c10, b).wait_recv())

        late = tau - LAG

        @when(ok(late + 2))
        def _():
            sent(c_core(late + 2, 0))

        @when(ok(late))
        def _():
            sent(c_a1(late))

        for go_right in (True, False):
            cb = late - z if go_right else late - 3 + z
            ca = late - 1 - z if go_right else late - 4 + z
            when(ok(cb))(lambda: b1(cb, go_right, sent, False))
            when(ok(ca))(lambda: a2(ca, go_right, sent, False))

        @when(ok(late - 3))
        def _():
            sent(c_b2(late - 3))

        @when(ok(late - 4))
        def _():
            sent(c_yo(late - 4))
            az(late - 4, z, sent, True)

        for k in (1, 2, 3):
            c = late - 4 - k
            for b, there in ((z - k, z - k >= 0), (z + k, z + k <= 3)):

                @when(ok(c), there)
                def _():
                    az(c, b, sent)
                    sent(c_ay(c, b))

        for k in (0, 1, 2, 3):
            c = late - 5 - k
            for b, there in ((z - k, z - k >= 0), (z + k, z + k <= 3))[: 1 if k == 0 else 2]:

                @when(ok(c), there)
                def _():
                    bz(c, b, sent)
                    sent(c_co(c, b))

    loop(0, N + 2 + 8 + LAG, step)
    for c in range(N - 4, N):
        for one in c_store(c):
            one.wait()


def whole_step(pieces, near, arrays):
    tiles = arrays[6].shape[1]
    T, N = tiles // pieces, 6 * pieces
    TA, TB = near, T - near
    tile = (16, 128)
    dma = pltpu.SemaphoreType.DMA
    scratch = [
        pltpu.VMEM((RING, 2, 4, T, *tile), BF16),
        pltpu.VMEM((N, 2, 4, T, *tile), BF16),
        pltpu.VMEM((N, 4, TA, *tile), BF16),
        pltpu.VMEM((N, 3, TA, *tile), BF16),
        pltpu.VMEM((N, 3, TA, *tile), BF16),
        pltpu.VMEM((N, 3, 2, TB, *tile), BF16),
        pltpu.VMEM((N, 3, 2, TB, *tile), BF16),
        pltpu.VMEM((N, TB, *tile), BF16),
        pltpu.VMEM((RING, T, *tile), BF16),
        pltpu.VMEM((4, T, *tile), BF16),
        pltpu.VMEM((4, T, *tile), F32),
        pltpu.VMEM((4, T, *tile), F32),
        pltpu.VMEM((T, *tile), BF16),
        dma((RING,)), dma((4, 3)), dma((4, 2)), dma((RING,)),
        dma((N,)), dma((N,)), dma((N, 3)), dma((N, 3)), dma((N, 3)), dma((N, 3)), dma((N,)), dma((N,)),
        dma((N, 4)), dma((N, 4)), dma((N, 4)), dma((N, 4)),
        dma((RING,)), dma((RING,)), dma((RING, 3)), dma((RING, 3)), dma((RING, 3)), dma((RING, 3)), dma((RING,)), dma((RING,)),
        dma((RING, 4)), dma((RING, 4)), dma((RING, 4)), dma((RING, 4)), dma((RING, 4)), dma((RING, 4)),
    ]

    def body(*refs):
        kernel(pieces, tiles, near, refs[:12], refs[12:15], refs[15:])

    hbm = pl.BlockSpec(memory_space=pl.ANY)
    return pl.pallas_call(
        body,
        out_shape=(
            jax.ShapeDtypeStruct((3, 2, 2, 4, 2, tiles, *tile), BF16),
            jax.ShapeDtypeStruct((3, 2, tiles, *tile), F32),
            jax.ShapeDtypeStruct((3, 2, tiles, *tile), F32),
        ),
        in_specs=[hbm] * 12,
        out_specs=(hbm,) * 3,
        scratch_shapes=scratch,
        compiler_params=pltpu.CompilerParams(collective_id=0, has_side_effects=True, vmem_limit_bytes=63 << 20),
    )(*arrays)


def to_tiles(a):
    _, r, c = a.shape
    return a.reshape(2, r // 8, 8, c // 128, 128).swapaxes(2, 3).reshape(2, -1, 16, 128)


def from_tiles(a, shape):
    _, r, c = shape
    return a.reshape(2, r // 8, c // 128, 8, 128).swapaxes(2, 3).reshape(shape)


def solution(mesh):
    def step(*arrays):
        arrays = [a.reshape(a.shape[-3:]) for a in arrays]
        tiled = [to_tiles(a) for a in arrays]
        blocks = tiled[6].shape[1]
        tiled = [t.reshape(2, 2, 4, 2, blocks, 16, 128) for t in tiled[:6]] + tiled[6:]
        w, m, v = whole_step(PIECES, 6 * blocks // (10 * PIECES), tiled)
        shapes, own = [a.shape for a in arrays[3:6]], [a.shape for a in arrays[6:9]]
        return (
            *(from_tiles(w[i], shapes[i]) for i in range(3)),
            *(from_tiles(m[i], own[i]) for i in range(3)),
            *(from_tiles(v[i], own[i]) for i in range(3)),
        )

    all_of, cut = P(None, None, None), P(None, "dp", None)
    return jax.shard_map(
        step,
        mesh=mesh,
        in_specs=(P(("rep", "dp"), None, None, None),) * 3 + (all_of,) * 3 + (cut,) * 6,
        out_specs=(P("rep", None, None),) * 3 + (P("rep", "dp", None),) * 6,
        check_vma=False,
    )
```

```python
import functools

import jax
import jax.numpy as jnp
from jax import lax
from jax.experimental import pallas as pl
from jax.experimental.pallas import tpu as pltpu
from jax.sharding import PartitionSpec as P

PIECES = 10
RING = 8
LAND = 16
LAG = 4
VMEM_LIMIT = 15 << 20
F32, BF16 = jnp.float32, jnp.bfloat16


def kernel(pieces, tiles, near, refs_in, refs_out, scratch):
    g_in, w_in, m_in, v_in = (refs_in[i : i + 3] for i in (0, 3, 6, 9))
    m_out, v_out, out = refs_out
    (G, CL, A1, AL, AR, BL, BR, B2, W, GS) = scratch[:10]
    (l_g, l_mv) = scratch[10:12]
    (r_core, r_a1, r_al, r_ar, r_bl, r_br, r_b2, r_yo, r_az, r_ay, r_bz, r_co) = scratch[12:24]
    (s_core, s_a1, s_al, s_ar, s_bl, s_br, s_b2, s_yo, s_azr, s_azl, s_ay, s_bzr, s_bzl, s_co) = scratch[24:]
    T = tiles // pieces
    TA, TB = near, T - near
    N = 6 * pieces
    x, me = lax.axis_index("rep"), lax.axis_index("dp")
    core, z, y = me % 2, (me // 2) % 4, me // 8
    partner, right, left, across = me + 1 - 2 * core, me + 2, me - 2, me + 8 - 16 * y

    barrier = pltpu.get_barrier_semaphore()

    def greet(device):
        pl.semaphore_signal(barrier, inc=1, device_id=(x, device), device_id_type=pl.DeviceIdType.MESH)

    greet(partner)
    greet(across)

    @pl.when(z > 0)
    def _():
        greet(left)

    @pl.when(z < 3)
    def _():
        greet(right)

    pl.semaphore_wait(barrier, 2 + jnp.where(z > 0, 1, 0) + jnp.where(z < 3, 1, 0))

    def copy(src, dst, ss, rs, device):
        return pltpu.make_async_remote_copy(
            src_ref=src, dst_ref=dst, send_sem=ss, recv_sem=rs, device_id=(x, device), device_id_type=pl.DeviceIdType.MESH
        )

    def place(c):
        w = c // (2 * pieces)
        r = c - w * 2 * pieces
        layer = r // pieces
        return w, layer, (r - layer * pieces) * T

    both, row, near_part, far_part = pl.ds(0, 2), pl.ds(0, 4), pl.ds(0, TA), pl.ds(TA, TB)

    def c_core(c, i):
        _, layer, at = place(c)
        src = g_in[i].at[layer, both, row, 1 - core, pl.ds(at, T)]
        return copy(src, CL.at[c % LAND], s_core.at[c % RING], r_core.at[c % LAND], partner)

    def c_g(c, i):
        _, layer, at = place(c)
        return pltpu.make_async_copy(g_in[i].at[layer, both, row, core, pl.ds(at, T)], G.at[c % RING], l_g.at[c % RING])

    def c_load(c, i):
        w, layer, at = place(c)
        k = c % 4
        return (
            pltpu.make_async_copy(m_in[i].at[layer, pl.ds(at, T)], m_out.at[w, layer, pl.ds(at, T)], l_mv.at[k, 0]),
            pltpu.make_async_copy(v_in[i].at[layer, pl.ds(at, T)], v_out.at[w, layer, pl.ds(at, T)], l_mv.at[k, 1]),
            pltpu.make_async_copy(w_in[i].at[layer, y, z, core, pl.ds(at, T)], W.at[k], l_mv.at[k, 2]),
        )

    def c_a1(c):
        return copy(CL.at[c % LAND, 1 - y, row, near_part], A1.at[c % LAND], s_a1.at[c % RING], r_a1.at[c % LAND], across)

    def c_a2(c, b, go_right):
        land, rs, ss, k, device = (AL, r_al, s_al, b - 1, right) if go_right else (AR, r_ar, s_ar, b, left)
        return copy(CL.at[c % LAND, y, b, near_part], land.at[c % LAND, k], ss.at[c % RING, k], rs.at[c % LAND, k], device)

    def c_b1(c, b, go_right):
        land, rs, ss, k, device = (BL, r_bl, s_bl, b - 1, right) if go_right else (BR, r_br, s_br, b, left)
        return copy(CL.at[c % LAND, both, b, far_part], land.at[c % LAND, k], ss.at[c % RING, k], rs.at[c % LAND, k], device)

    def c_b2(c):
        return copy(CL.at[c % LAND, 1 - y, z, far_part], B2.at[c % LAND], s_b2.at[c % RING], r_b2.at[c % LAND], across)

    def spot(c, rows, column, at, n):
        w, layer, start = place(c)
        return out.at[w, layer, rows, column, core, pl.ds(start + at, n)]

    def c_yo(c):
        return copy(spot(c, y, z, 0, T), spot(c, y, z, 0, T), s_yo.at[c % RING], r_yo.at[c % LAND], across)

    def c_az(c, b, go_right):
        ss, device = (s_azr, right) if go_right else (s_azl, left)
        return copy(spot(c, y, b, 0, TA), spot(c, y, b, 0, TA), ss.at[c % RING, b], r_az.at[c % LAND, b], device)

    def c_ay(c, b):
        return copy(spot(c, y, b, 0, TA), spot(c, y, b, 0, TA), s_ay.at[c % RING, b], r_ay.at[c % LAND, b], across)

    def c_bz(c, b, go_right):
        ss, device = (s_bzr, right) if go_right else (s_bzl, left)
        return copy(spot(c, both, b, TA, TB), spot(c, both, b, TA, TB), ss.at[c % RING, b], r_bz.at[c % LAND, b], device)

    def c_co(c, b):
        return copy(spot(c, both, b, 0, T), spot(c, both, b, 0, T), s_co.at[c % RING, b], r_co.at[c % LAND, b], partner)

    def start(copies):
        for one in copies if isinstance(copies, tuple) else (copies,):
            one.start()

    def sent(one):
        one.wait_send()

    def ok(c):
        return jnp.logical_and(c >= 0, c < N)

    def when(*conds):
        return pl.when(functools.reduce(jnp.logical_and, conds))

    def loop(low, high, body):
        lax.fori_loop(low, high, lambda i, _: (body(i), 0)[1], 0)

    def of_weight(c, do):
        w = c // (2 * pieces)
        for i in range(3):

            @pl.when(w == i)
            def _():
                do(i)

    def total(terms):
        return functools.reduce(jnp.add, (one.astype(F32) for one in terms))

    def a2(c, go_right, act, sums):
        def one(b):
            if sums:

                def put(inner):
                    terms = [G[c % RING, y, b, near_part], CL[c % LAND, y, b, near_part], A1[c % LAND, b]]
                    if inner:
                        terms.append(AL[c % LAND, b - 1] if go_right else AR[c % LAND, b])
                    CL[c % LAND, y, b, near_part] = total(terms).astype(BF16)

                pl.when(z == (0 if go_right else 3))(lambda: put(False))
                pl.when(z != (0 if go_right else 3))(lambda: put(True))
            act(c_a2(c, b, go_right))

        loop(z + 1, 4, one) if go_right else loop(0, z, one)

    def b1(c, go_right, act, sums):
        def one(b):
            if sums:

                def put(inner):
                    terms = [G[c % RING, both, b, far_part], CL[c % LAND, both, b, far_part]]
                    if inner:
                        terms.append(BL[c % LAND, b - 1] if go_right else BR[c % LAND, b])
                    CL[c % LAND, both, b, far_part] = total(terms).astype(BF16)

                pl.when(z == (0 if go_right else 3))(lambda: put(False))
                pl.when(z != (0 if go_right else 3))(lambda: put(True))
            act(c_b1(c, b, go_right))

        loop(z + 1, 4, one) if go_right else loop(0, z, one)

    def arrived(c, go_right, make):
        if go_right:
            when(z > 0)(lambda: loop(z, 4, lambda b: make(c, b, True).wait_recv()))
        else:
            when(z < 3)(lambda: loop(0, z + 1, lambda b: make(c, b, False).wait_recv()))

    def own_part(c, yy, part, with_rows, land_l, land_r, extra, put):
        def terms():
            return [G[c % RING, yy, z, part], CL[c % LAND, yy, z, part], *extra()]

        def from_left():
            return land_l[c % LAND, z - 1, yy] if with_rows else land_l[c % LAND, z - 1]

        def from_right():
            return land_r[c % LAND, z, yy] if with_rows else land_r[c % LAND, z]

        pl.when(z == 0)(lambda: put(total([*terms(), from_right()])))
        pl.when(z == 3)(lambda: put(total([*terms(), from_left()])))
        when(z > 0, z < 3)(lambda: put(total([*terms(), from_left(), from_right()])))

    def az(c, b, act):
        when(z < 3, b <= z)(lambda: act(c_az(c, b, True)))
        when(z > 0, b >= z)(lambda: act(c_az(c, b, False)))

    def bz(c, b, act):
        when(z < 3, b <= z)(lambda: act(c_bz(c, b, True)))
        when(z > 0, b >= z)(lambda: act(c_bz(c, b, False)))

    def step(t):
        @pl.when(t < N)
        def _():
            of_weight(t, lambda i: (start(c_core(t, i)), start(c_g(t, i))))

        c0 = t - 4

        @when(ok(c0))
        def _():
            of_weight(c0, lambda i: start(c_load(c0, i)))

        tau = t - 2

        @when(ok(tau))
        def _():
            c_g(tau, 0).wait()
            c_core(tau, 0).wait_recv()

            def add(b):
                CL[tau % LAND, 1 - y, b, near_part] = total((G[tau % RING, 1 - y, b, near_part], CL[tau % LAND, 1 - y, b, near_part])).astype(BF16)

            loop(0, 4, add)
            c_a1(tau).start()

        for go_right in (True, False):
            c = tau - z if go_right else tau - 3 + z

            @when(ok(c))
            def _():
                arrived(c, go_right, c_b1)
                b1(c, go_right, start, True)

        @when(ok(tau - 1))
        def _():
            c_a1(tau - 1).wait_recv()

        for go_right in (True, False):
            c = tau - 1 - z if go_right else tau - 4 + z

            @when(ok(c))
            def _():
                arrived(c, go_right, c_a2)
                a2(c, go_right, start, True)

        c3 = tau - 3

        @when(ok(c3))
        def _():
            def put(value):
                CL[c3 % LAND, 1 - y, z, far_part] = value.astype(BF16)

            own_part(c3, 1 - y, far_part, True, BL, BR, lambda: (), put)
            c_b2(c3).start()

        c4 = tau - 4

        @when(ok(c4))
        def _():
            c_b2(c4).wait_recv()
            for one in c_load(c4, 0):
                one.wait()

            def put_near(value):
                GS[near_part] = value.astype(BF16)

            def put_far(value):
                GS[far_part] = value.astype(BF16)

            own_part(c4, y, near_part, False, AL, AR, lambda: (A1[c4 % LAND, z],), put_near)
            own_part(c4, y, far_part, True, BL, BR, lambda: (B2[c4 % LAND],), put_far)
            i, layer, at = place(c4)
            here = pl.ds(at, T)
            g = GS[...].astype(F32)
            m = 0.9 * m_out[i, layer, here] + 0.1 * g
            v = 0.95 * v_out[i, layer, here] + 0.05 * g * g
            w = W[c4 % 4].astype(F32)
            out[i, layer, y, z, core, here] = (w - 0.02 * (m * lax.rsqrt(v + 1e-8) + 0.1 * w)).astype(BF16)
            m_out[i, layer, here] = m
            v_out[i, layer, here] = v
            c_yo(c4).start()
            az(c4, z, start)

        for k in (1, 2, 3):
            c = tau - 4 - k
            for b, there in ((z - k, z - k >= 0), (z + k, z + k <= 3)):

                @when(ok(c), there)
                def _():
                    c_az(c, b, True).wait_recv()
                    az(c, b, start)
                    c_ay(c, b).start()

        for k in (0, 1, 2, 3):
            c = tau - 5 - k
            for b, there in ((z - k, z - k >= 0), (z + k, z + k <= 3))[: 1 if k == 0 else 2]:

                @when(ok(c), there)
                def _():
                    if k == 0:
                        c_yo(c).wait_recv()
                    else:
                        c_bz(c, b, True).wait_recv()
                        c_ay(c, b).wait_recv()
                    bz(c, b, start)
                    c_co(c, b).start()

        c10 = tau - 10

        @when(ok(c10))
        def _():
            loop(0, 4, lambda b: c_co(c10, b).wait_recv())

        late = tau - LAG

        @when(ok(late + 2))
        def _():
            sent(c_core(late + 2, 0))

        @when(ok(late))
        def _():
            sent(c_a1(late))

        for go_right in (True, False):
            cb = late - z if go_right else late - 3 + z
            ca = late - 1 - z if go_right else late - 4 + z
            when(ok(cb))(lambda: b1(cb, go_right, sent, False))
            when(ok(ca))(lambda: a2(ca, go_right, sent, False))

        @when(ok(late - 3))
        def _():
            sent(c_b2(late - 3))

        @when(ok(late - 4))
        def _():
            sent(c_yo(late - 4))
            az(late - 4, z, sent)

        for k in (1, 2, 3):
            c = late - 4 - k
            for b, there in ((z - k, z - k >= 0), (z + k, z + k <= 3)):

                @when(ok(c), there)
                def _():
                    az(c, b, sent)
                    sent(c_ay(c, b))

        for k in (0, 1, 2, 3):
            c = late - 5 - k
            for b, there in ((z - k, z - k >= 0), (z + k, z + k <= 3))[: 1 if k == 0 else 2]:

                @when(ok(c), there)
                def _():
                    bz(c, b, sent)
                    sent(c_co(c, b))

    loop(0, N + 2 + 8 + LAG, step)


def whole_step(pieces, near, arrays):
    tiles = arrays[6].shape[1]
    T, N = tiles // pieces, 6 * pieces
    TA, TB = near, T - near
    tile = (16, 128)
    dma = pltpu.SemaphoreType.DMA
    scratch = [
        pltpu.VMEM((RING, 2, 4, T, *tile), BF16),
        pltpu.VMEM((LAND, 2, 4, T, *tile), BF16),
        pltpu.VMEM((LAND, 4, TA, *tile), BF16),
        pltpu.VMEM((LAND, 3, TA, *tile), BF16),
        pltpu.VMEM((LAND, 3, TA, *tile), BF16),
        pltpu.VMEM((LAND, 3, 2, TB, *tile), BF16),
        pltpu.VMEM((LAND, 3, 2, TB, *tile), BF16),
        pltpu.VMEM((LAND, TB, *tile), BF16),
        pltpu.VMEM((4, T, *tile), BF16),
        pltpu.VMEM((T, *tile), BF16),
        dma((RING,)), dma((4, 3)),
        dma((LAND,)), dma((LAND,)), dma((LAND, 3)), dma((LAND, 3)), dma((LAND, 3)), dma((LAND, 3)), dma((LAND,)), dma((LAND,)),
        dma((LAND, 4)), dma((LAND, 4)), dma((LAND, 4)), dma((LAND, 4)),
        dma((RING,)), dma((RING,)), dma((RING, 3)), dma((RING, 3)), dma((RING, 3)), dma((RING, 3)), dma((RING,)), dma((RING,)),
        dma((RING, 4)), dma((RING, 4)), dma((RING, 4)), dma((RING, 4)), dma((RING, 4)), dma((RING, 4)),
    ]

    def body(*refs):
        kernel(pieces, tiles, near, refs[:12], refs[12:15], refs[15:])

    hbm, vmem = (pl.BlockSpec(memory_space=space) for space in (pl.ANY, pltpu.VMEM))
    return pl.pallas_call(
        body,
        out_shape=(
            pltpu.VMEM((3, 2, tiles, *tile), F32),
            pltpu.VMEM((3, 2, tiles, *tile), F32),
            pltpu.VMEM((3, 2, 2, 4, 2, tiles, *tile), BF16),
        ),
        in_specs=[hbm] * 12,
        out_specs=(vmem,) * 3,
        scratch_shapes=scratch,
        compiler_params=pltpu.CompilerParams(collective_id=0, has_side_effects=True, vmem_limit_bytes=VMEM_LIMIT),
    )(*arrays)


def unload(w, m, v):
    def body(*refs):
        given, outs, sems = refs[:3], refs[3:12], refs[12]
        copies = [pltpu.make_async_copy(given[i // 3].at[i % 3], outs[i], sems.at[i]) for i in range(9)]
        for one in copies:
            one.start()
        for one in copies:
            one.wait()

    given = [pltpu.with_memory_space_constraint(a, pltpu.VMEM) for a in (w, m, v)]
    return pl.pallas_call(
        body,
        out_shape=tuple(jax.ShapeDtypeStruct(a.shape[1:], a.dtype) for a in (w, m, v) for _ in range(3)),
        in_specs=[pl.BlockSpec(memory_space=pltpu.VMEM)] * 3,
        out_specs=(pl.BlockSpec(memory_space=pl.ANY),) * 9,
        scratch_shapes=[pltpu.SemaphoreType.DMA((9,))],
        compiler_params=pltpu.CompilerParams(vmem_limit_bytes=1 << 20),
    )(*given)


def to_tiles(a):
    _, r, c = a.shape
    return a.reshape(2, r // 8, 8, c // 128, 128).swapaxes(2, 3).reshape(2, -1, 16, 128)


def from_tiles(a, shape):
    _, r, c = shape
    return a.reshape(2, r // 8, c // 128, 8, 128).swapaxes(2, 3).reshape(shape)


def solution(mesh):
    def step(*arrays):
        arrays = [a.reshape(a.shape[-3:]) for a in arrays]
        tiled = [to_tiles(a) for a in arrays]
        blocks = tiled[6].shape[1]
        tiled = [t.reshape(2, 2, 4, 2, blocks, 16, 128) for t in tiled[:6]] + tiled[6:]
        results = unload(*(lambda r: (r[2], r[0], r[1]))(whole_step(PIECES, 6 * blocks // (10 * PIECES), tiled)))
        shapes = [a.shape for a in arrays[3:9]] + [a.shape for a in arrays[6:9]]
        return tuple(from_tiles(one, shape) for one, shape in zip(results, shapes, strict=True))

    all_of, cut = P(None, None, None), P(None, "dp", None)
    return jax.shard_map(
        step,
        mesh=mesh,
        in_specs=(P(("rep", "dp"), None, None, None),) * 3 + (all_of,) * 3 + (cut,) * 6,
        out_specs=(P("rep", None, None),) * 3 + (P("rep", "dp", None),) * 6,
        check_vma=False,
    )
```

```python
import functools

import jax
import jax.numpy as jnp
from jax import lax
from jax.experimental import pallas as pl
from jax.experimental.pallas import tpu as pltpu
from jax.sharding import PartitionSpec as P

PIECES = 10
LAND = 16
RING = 8
LAG = 3
SENDS = 4
VMEM_LIMIT = 15 << 20
F32, BF16 = jnp.float32, jnp.bfloat16


class Chunk:
    def __init__(self, c, count):
        self.c = c
        self.ok = jnp.logical_and(c >= 0, c < count)
        self.s, self.g, self.k = (lax.rem(c + 64, n) for n in (SENDS, RING, LAND))


def kernel(pieces, tiles, near, refs_in, refs_out, scratch):
    g_in, w_in, m_in, v_in = (refs_in[i : i + 3] for i in (0, 3, 6, 9))
    m_out, v_out, out = refs_out
    (G, CL, A1, AL, AR, BL, BR, B2, W, GS) = scratch[:10]
    (l_g, l_mv) = scratch[10:12]
    (r_core, r_a1, r_al, r_ar, r_bl, r_br, r_b2, r_yo, r_az, r_ay, r_bz, r_co) = scratch[12:24]
    (s_core, s_a1, s_al, s_ar, s_bl, s_br, s_b2, s_yo, s_azr, s_azl, s_ay, s_bzr, s_bzl, s_co) = scratch[24:]
    T = tiles // pieces
    TA, TB = near, T - near
    N = 6 * pieces
    x, me = lax.axis_index("rep"), lax.axis_index("dp")
    core, z, y = me % 2, (me // 2) % 4, me // 8
    partner, right, left, across = me + 1 - 2 * core, me + 2, me - 2, me + 8 - 16 * y

    barrier = pltpu.get_barrier_semaphore()

    def greet(device):
        pl.semaphore_signal(barrier, inc=1, device_id=(x, device), device_id_type=pl.DeviceIdType.MESH)

    greet(partner)
    greet(across)

    @pl.when(z > 0)
    def _():
        greet(left)

    @pl.when(z < 3)
    def _():
        greet(right)

    pl.semaphore_wait(barrier, 2 + jnp.where(z > 0, 1, 0) + jnp.where(z < 3, 1, 0))

    def copy(src, dst, ss, rs, device):
        return pltpu.make_async_remote_copy(
            src_ref=src, dst_ref=dst, send_sem=ss, recv_sem=rs, device_id=(x, device), device_id_type=pl.DeviceIdType.MESH
        )

    both, row, near_part, far_part, whole = pl.ds(0, 2), pl.ds(0, 4), pl.ds(0, TA), pl.ds(TA, TB), pl.ds(0, T)

    def place(c):
        layers = lax.div(c, pieces)
        return lax.rem(layers, 2), pl.ds((c - layers * pieces) * T, T)

    def c_core(n, i):
        layer, at = place(n.c)
        return copy(g_in[i].at[layer, both, row, 1 - core, at], CL.at[n.k], s_core.at[n.s], r_core.at[n.g], partner)

    def c_g(n, i):
        layer, at = place(n.c)
        return pltpu.make_async_copy(g_in[i].at[layer, both, row, core, at], G.at[n.g], l_g.at[n.s])

    def c_load(n, i):
        layer, at = place(n.c)
        return (
            pltpu.make_async_copy(m_in[i].at[layer, at], m_out.at[n.c], l_mv.at[n.s, 0]),
            pltpu.make_async_copy(v_in[i].at[layer, at], v_out.at[n.c], l_mv.at[n.s, 1]),
            pltpu.make_async_copy(w_in[i].at[layer, y, z, core, at], W.at[n.s], l_mv.at[n.s, 2]),
        )

    def c_a1(n):
        return copy(CL.at[n.k, 1 - y, row, near_part], A1.at[n.k], s_a1.at[n.s], r_a1.at[n.s], across)

    def c_a2(n, b, go_right):
        land, rs, ss, j, device = (AL, r_al, s_al, b - 1, right) if go_right else (AR, r_ar, s_ar, b, left)
        return copy(CL.at[n.k, y, b, near_part], land.at[n.k, j], ss.at[n.s, j], rs.at[n.s, j], device)

    def c_b1(n, b, go_right):
        land, rs, ss, j, device = (BL, r_bl, s_bl, b - 1, right) if go_right else (BR, r_br, s_br, b, left)
        return copy(CL.at[n.k, both, b, far_part], land.at[n.k, j], ss.at[n.s, j], rs.at[n.s, j], device)

    def c_b2(n):
        return copy(CL.at[n.k, 1 - y, z, far_part], B2.at[n.k], s_b2.at[n.s], r_b2.at[n.s], across)

    def same(n, rows, column, part, ss, rs, device):
        there = out.at[n.c, rows, column, core, part]
        return copy(there, there, ss, rs, device)

    def c_yo(n):
        return same(n, y, z, whole, s_yo.at[n.s], r_yo.at[n.s], across)

    def c_az(n, b, go_right):
        ss, device = (s_azr, right) if go_right else (s_azl, left)
        return same(n, y, b, near_part, ss.at[n.s, b], r_az.at[n.s, b], device)

    def c_ay(n, b):
        return same(n, y, b, near_part, s_ay.at[n.s, b], r_ay.at[n.s, b], across)

    def c_bz(n, b, go_right):
        ss, device = (s_bzr, right) if go_right else (s_bzl, left)
        return same(n, both, b, far_part, ss.at[n.s, b], r_bz.at[n.s, b], device)

    def c_co(n, b):
        return same(n, both, b, whole, s_co.at[n.s, b], r_co.at[n.k], partner)

    def c_co_all(n):
        return same(n, both, row, whole, s_co.at[n.s, 0], r_co.at[n.k], partner)

    def start(copies):
        for one in copies if isinstance(copies, tuple) else (copies,):
            one.start()

    def sent(one):
        one.wait_send()

    def when(*conds):
        return pl.when(functools.reduce(jnp.logical_and, conds))

    def loop(low, high, body):
        lax.fori_loop(low, high, lambda i, _: (body(i), 0)[1], 0)

    def of_weight(n, do):
        for i in range(3):
            when(n.c >= 2 * i * pieces, n.c < 2 * (i + 1) * pieces)(functools.partial(do, i))

    def total(terms):
        return functools.reduce(jnp.add, (one.astype(F32) for one in terms))

    def a2(n, go_right, act, sums):
        def one(b):
            if sums:

                def put(inner):
                    terms = [G[n.g, y, b, near_part], CL[n.k, y, b, near_part], A1[n.k, b]]
                    if inner:
                        terms.append(AL[n.k, b - 1] if go_right else AR[n.k, b])
                    CL[n.k, y, b, near_part] = total(terms).astype(BF16)

                pl.when(z == (0 if go_right else 3))(lambda: put(False))
                pl.when(z != (0 if go_right else 3))(lambda: put(True))
            act(c_a2(n, b, go_right))

        loop(z + 1, 4, one) if go_right else loop(0, z, one)

    def b1(n, go_right, act, sums):
        def one(b):
            if sums:

                def put(inner):
                    terms = [G[n.g, both, b, far_part], CL[n.k, both, b, far_part]]
                    if inner:
                        terms.append(BL[n.k, b - 1] if go_right else BR[n.k, b])
                    CL[n.k, both, b, far_part] = total(terms).astype(BF16)

                pl.when(z == (0 if go_right else 3))(lambda: put(False))
                pl.when(z != (0 if go_right else 3))(lambda: put(True))
            act(c_b1(n, b, go_right))

        loop(z + 1, 4, one) if go_right else loop(0, z, one)

    def arrived(n, go_right, make):
        if go_right:
            when(z > 0)(lambda: loop(z, 4, lambda b: make(n, b, True).wait_recv()))
        else:
            when(z < 3)(lambda: loop(0, z + 1, lambda b: make(n, b, False).wait_recv()))

    def own_part(n, yy, part, with_rows, land_l, land_r, extra, put):
        def terms():
            return [G[n.g, yy, z, part], CL[n.k, yy, z, part], *extra()]

        def from_left():
            return land_l[n.k, z - 1, yy] if with_rows else land_l[n.k, z - 1]

        def from_right():
            return land_r[n.k, z, yy] if with_rows else land_r[n.k, z]

        pl.when(z == 0)(lambda: put(total([*terms(), from_right()])))
        pl.when(z == 3)(lambda: put(total([*terms(), from_left()])))
        when(z > 0, z < 3)(lambda: put(total([*terms(), from_left(), from_right()])))

    def az(n, b, act):
        when(z < 3, b <= z)(lambda: act(c_az(n, b, True)))
        when(z > 0, b >= z)(lambda: act(c_az(n, b, False)))

    def bz(n, b, act):
        when(z < 3, b <= z)(lambda: act(c_bz(n, b, True)))
        when(z > 0, b >= z)(lambda: act(c_bz(n, b, False)))

    def sides(k):
        return ((z, z >= 0),) if k == 0 else ((z - k, z >= k), (z + k, z <= 3 - k))

    def step(t):
        tau = t - 2
        back = [Chunk(tau - k, N) for k in range(9 + LAG)]
        inward = {
            (late, kind, go_right): Chunk(tau - late - kind - (z if go_right else 3 - z), N)
            for late in (0, LAG)
            for kind in (0, 1)
            for go_right in (True, False)
        }
        first, ahead, last = Chunk(t, N), Chunk(t - 4, N), Chunk(tau - 10, N)

        @pl.when(first.ok)
        def _():
            of_weight(first, lambda i: (start(c_core(first, i)), start(c_g(first, i)), None)[2])

        @pl.when(ahead.ok)
        def _():
            of_weight(ahead, lambda i: start(c_load(ahead, i)))

        n0 = back[0]

        @pl.when(n0.ok)
        def _():
            c_g(n0, 0).wait()
            c_core(n0, 0).wait_recv()
            CL[n0.k, 1 - y, row, near_part] = total((G[n0.g, 1 - y, row, near_part], CL[n0.k, 1 - y, row, near_part])).astype(BF16)
            c_a1(n0).start()

        for go_right in (True, False):
            n = inward[0, 0, go_right]

            @pl.when(n.ok)
            def _():
                arrived(n, go_right, c_b1)
                b1(n, go_right, start, True)

        @pl.when(back[1].ok)
        def _():
            c_a1(back[1]).wait_recv()

        for go_right in (True, False):
            n = inward[0, 1, go_right]

            @pl.when(n.ok)
            def _():
                arrived(n, go_right, c_a2)
                a2(n, go_right, start, True)

        n3 = back[3]

        @pl.when(n3.ok)
        def _():
            def put(value):
                CL[n3.k, 1 - y, z, far_part] = value.astype(BF16)

            own_part(n3, 1 - y, far_part, True, BL, BR, lambda: (), put)
            c_b2(n3).start()

        n4 = back[4]

        @pl.when(n4.ok)
        def _():
            c_b2(n4).wait_recv()
            for one in c_load(n4, 0):
                one.wait()

            def put_near(value):
                GS[near_part] = value.astype(BF16)

            def put_far(value):
                GS[far_part] = value.astype(BF16)

            own_part(n4, y, near_part, False, AL, AR, lambda: (A1[n4.k, z],), put_near)
            own_part(n4, y, far_part, True, BL, BR, lambda: (B2[n4.k],), put_far)
            g = GS[...].astype(F32)
            m = 0.9 * m_out[n4.c] + 0.1 * g
            v = 0.95 * v_out[n4.c] + 0.05 * g * g
            w = W[n4.s].astype(F32)
            out[n4.c, y, z, core] = (w - 0.02 * (m * lax.rsqrt(v + 1e-8) + 0.1 * w)).astype(BF16)
            m_out[n4.c] = m
            v_out[n4.c] = v
            c_yo(n4).start()
            az(n4, z, start)

        for k in (1, 2, 3):
            n = back[4 + k]
            for b, there in sides(k):

                @when(n.ok, there)
                def _():
                    c_az(n, b, True).wait_recv()
                    az(n, b, start)
                    c_ay(n, b).start()

        for k in (0, 1, 2, 3):
            n = back[5 + k]
            for b, there in sides(k):

                @when(n.ok, there)
                def _():
                    if k == 0:
                        c_yo(n).wait_recv()
                    else:
                        c_bz(n, b, True).wait_recv()
                        c_ay(n, b).wait_recv()
                    bz(n, b, start)
                    c_co(n, b).start()

        @pl.when(last.ok)
        def _():
            c_co_all(last).wait_recv()

        @pl.when(back[LAG].ok)
        def _():
            sent(c_core(back[LAG], 0))
            sent(c_a1(back[LAG]))

        for go_right in (True, False):
            for kind, group in enumerate((b1, a2)):
                n = inward[LAG, kind, go_right]
                pl.when(n.ok)(functools.partial(group, n, go_right, sent, False))

        @pl.when(back[LAG + 3].ok)
        def _():
            sent(c_b2(back[LAG + 3]))

        @pl.when(back[LAG + 4].ok)
        def _():
            sent(c_yo(back[LAG + 4]))
            az(back[LAG + 4], z, sent)

        for k in (1, 2, 3):
            n = back[LAG + 4 + k]
            for b, there in sides(k):

                @when(n.ok, there)
                def _():
                    az(n, b, sent)
                    sent(c_ay(n, b))

        for k in (0, 1, 2, 3):
            n = back[LAG + 5 + k]
            for b, there in sides(k):

                @when(n.ok, there)
                def _():
                    bz(n, b, sent)
                    sent(c_co(n, b))

    loop(0, N + 2 + 8 + LAG, step)


def whole_step(pieces, near, arrays):
    tiles = arrays[6].shape[1]
    T, N = tiles // pieces, 6 * pieces
    TA, TB = near, T - near
    tile = (16, 128)
    dma = pltpu.SemaphoreType.DMA
    scratch = [
        pltpu.VMEM((RING, 2, 4, T, *tile), BF16),
        pltpu.VMEM((LAND, 2, 4, T, *tile), BF16),
        pltpu.VMEM((LAND, 4, TA, *tile), BF16),
        pltpu.VMEM((LAND, 3, TA, *tile), BF16),
        pltpu.VMEM((LAND, 3, TA, *tile), BF16),
        pltpu.VMEM((LAND, 3, 2, TB, *tile), BF16),
        pltpu.VMEM((LAND, 3, 2, TB, *tile), BF16),
        pltpu.VMEM((LAND, TB, *tile), BF16),
        pltpu.VMEM((SENDS, T, *tile), BF16),
        pltpu.VMEM((T, *tile), BF16),
        dma((SENDS,)), dma((SENDS, 3)),
        dma((RING,)), dma((SENDS,)), dma((SENDS, 3)), dma((SENDS, 3)), dma((SENDS, 3)), dma((SENDS, 3)), dma((SENDS,)), dma((SENDS,)),
        dma((SENDS, 4)), dma((SENDS, 4)), dma((SENDS, 4)), dma((LAND,)),
        dma((SENDS,)), dma((SENDS,)), dma((SENDS, 3)), dma((SENDS, 3)), dma((SENDS, 3)), dma((SENDS, 3)), dma((SENDS,)), dma((SENDS,)),
        dma((SENDS, 4)), dma((SENDS, 4)), dma((SENDS, 4)), dma((SENDS, 4)), dma((SENDS, 4)), dma((SENDS, 4)),
    ]

    def body(*refs):
        kernel(pieces, tiles, near, refs[:12], refs[12:15], refs[15:])

    hbm, vmem = (pl.BlockSpec(memory_space=space) for space in (pl.ANY, pltpu.VMEM))
    return pl.pallas_call(
        body,
        out_shape=(
            pltpu.VMEM((N, T, *tile), F32),
            pltpu.VMEM((N, T, *tile), F32),
            pltpu.VMEM((N, 2, 4, 2, T, *tile), BF16),
        ),
        in_specs=[hbm] * 12,
        out_specs=(vmem,) * 3,
        scratch_shapes=scratch,
        compiler_params=pltpu.CompilerParams(collective_id=0, has_side_effects=True, vmem_limit_bytes=VMEM_LIMIT),
    )(*arrays)


def unload(m, v, w):
    N, T, *tile = m.shape
    pieces = N // 6

    def body(m, v, w, *refs):
        outs, sems = refs[:9], refs[9]
        every = [pl.ds(0, n) for n in (2, 4, 2)]
        for i in range(3):
            for c in range(2 * pieces):
                there = outs[i].at[(c // pieces, *every, c % pieces)]
                pltpu.make_async_copy(w.at[2 * i * pieces + c], there, sems.at[i]).start()
            here = pl.ds(2 * i * pieces, 2 * pieces)
            pltpu.make_async_copy(m.at[here], outs[3 + i], sems.at[3 + i]).start()
            pltpu.make_async_copy(v.at[here], outs[6 + i], sems.at[6 + i]).start()
        for i in range(9):
            pltpu.make_async_copy(outs[i], outs[i], sems.at[i]).wait()

    given = [pltpu.with_memory_space_constraint(a, pltpu.VMEM) for a in (m, v, w)]
    return pl.pallas_call(
        body,
        out_shape=(jax.ShapeDtypeStruct((2, 2, 4, 2, pieces, T, *tile), BF16),) * 3
        + (jax.ShapeDtypeStruct((2 * pieces, T, *tile), F32),) * 6,
        in_specs=[pl.BlockSpec(memory_space=pltpu.VMEM)] * 3,
        out_specs=(pl.BlockSpec(memory_space=pl.ANY),) * 9,
        scratch_shapes=[pltpu.SemaphoreType.DMA((9,))],
        compiler_params=pltpu.CompilerParams(vmem_limit_bytes=1 << 20),
    )(*given)


def to_tiles(a):
    _, r, c = a.shape
    return a.reshape(2, r // 8, 8, c // 128, 128).swapaxes(2, 3).reshape(2, -1, 16, 128)


def from_tiles(a, shape):
    _, r, c = shape
    return a.reshape(2, r // 8, c // 128, 8, 128).swapaxes(2, 3).reshape(shape)


def solution(mesh):
    def step(*arrays):
        arrays = [a.reshape(a.shape[-3:]) for a in arrays]
        tiled = [to_tiles(a) for a in arrays]
        blocks = tiled[6].shape[1]
        tiled = [t.reshape(2, 2, 4, 2, blocks, 16, 128) for t in tiled[:6]] + tiled[6:]
        results = unload(*whole_step(PIECES, 6 * blocks // (10 * PIECES), tiled))
        shapes = [a.shape for a in arrays[3:9]] + [a.shape for a in arrays[6:9]]
        return tuple(from_tiles(one, shape) for one, shape in zip(results, shapes, strict=True))

    all_of, cut = P(None, None, None), P(None, "dp", None)
    return jax.shard_map(
        step,
        mesh=mesh,
        in_specs=(P(("rep", "dp"), None, None, None),) * 3 + (all_of,) * 3 + (cut,) * 6,
        out_specs=(P("rep", None, None),) * 3 + (P("rep", "dp", None),) * 6,
        check_vma=False,
    )
```

```python
import functools
import itertools

import jax
import jax.numpy as jnp
from jax import lax
from jax.experimental import pallas as pl
from jax.experimental.pallas import tpu as pltpu
from jax.sharding import PartitionSpec as P

PIECES = 10
LAND = 16
RING = 8
LAG = 1
SENDS = 2
ARRIVALS = 4
VMEM_LIMIT = 15 << 20
F32, BF16 = jnp.float32, jnp.bfloat16


class Chunk:
    def __init__(self, c, count):
        self.c = c
        self.ok = jnp.logical_and(c >= 0, c < count)
        self.s, self.r, self.g, self.k = (lax.rem(c + 64, n) for n in (SENDS, ARRIVALS, RING, LAND))


def kernel(pieces, tiles, near, refs_in, refs_out, scratch):
    g_in, w_in, m_in, v_in = (refs_in[i : i + 3] for i in (0, 3, 6, 9))
    m_out, v_out, out = refs_out
    (G, CL, A1, AL, AR, BL, BR, B2, W, GS) = scratch[:10]
    (l_g, l_mv) = scratch[10:12]
    (r_core, r_a1, r_al, r_ar, r_bl, r_br, r_b2, r_yo, r_az, r_ay, r_bz, r_co) = scratch[12:24]
    (s_core, s_a1, s_al, s_ar, s_bl, s_br, s_b2, s_yo, s_azr, s_azl, s_ay, s_bzr, s_bzl, s_co) = scratch[24:]
    T = tiles // pieces
    TA, TB = near, T - near
    N = 6 * pieces
    x, me = lax.axis_index("rep"), lax.axis_index("dp")
    core, z, y = me % 2, (me // 2) % 4, me // 8
    plane, other = (core + y + z) % 2, 1 - 2 * core
    partner, right, left, across = me + other, me + 2 + other, me - 2 + other, me + 8 - 16 * y + other

    barrier = pltpu.get_barrier_semaphore()

    def greet(device):
        pl.semaphore_signal(barrier, inc=1, device_id=(x, device), device_id_type=pl.DeviceIdType.MESH)

    greet(partner)
    greet(across)

    @pl.when(z > 0)
    def _():
        greet(left)

    @pl.when(z < 3)
    def _():
        greet(right)

    pl.semaphore_wait(barrier, 2 + jnp.where(z > 0, 1, 0) + jnp.where(z < 3, 1, 0))

    def copy(src, dst, ss, rs, device):
        return pltpu.make_async_remote_copy(
            src_ref=src, dst_ref=dst, send_sem=ss, recv_sem=rs, device_id=(x, device), device_id_type=pl.DeviceIdType.MESH
        )

    both, row, near_part, far_part, whole = pl.ds(0, 2), pl.ds(0, 4), pl.ds(0, TA), pl.ds(TA, TB), pl.ds(0, T)

    def place(c):
        layers = lax.div(c, pieces)
        return lax.rem(layers, 2), pl.ds((c - layers * pieces) * T, T)

    def at_z(b):
        return 2 * lax.rem(b, 2) + lax.div(b, 2)

    def terms_of(n, i, which, slot):
        layer, at = place(n.c)
        for yy in range(2):
            for odd in range(2):
                its = which if yy == odd else 1 - which
                yield g_in[i].at[layer, yy, both, odd, its, at], slot.at[yy, pl.ds(2 * odd, 2)]

    def c_core(n, i):
        return tuple(copy(src, dst, s_core.at[n.r], r_core.at[n.g], partner) for src, dst in terms_of(n, i, 1 - plane, CL.at[n.k]))

    def c_core_all(n):
        return copy(CL.at[n.k], CL.at[n.k], s_core.at[n.r], r_core.at[n.g], partner)

    def c_g(n, i):
        return tuple(pltpu.make_async_copy(src, dst, l_g.at[n.r]) for src, dst in terms_of(n, i, plane, G.at[n.g]))

    def c_g_all(n):
        return pltpu.make_async_copy(G.at[n.g], G.at[n.g], l_g.at[n.r])

    def c_load(n, i):
        layer, at = place(n.c)
        return (
            pltpu.make_async_copy(m_in[i].at[layer, at], m_out.at[n.c], l_mv.at[n.r, 0]),
            pltpu.make_async_copy(v_in[i].at[layer, at], v_out.at[n.c], l_mv.at[n.r, 1]),
            pltpu.make_async_copy(w_in[i].at[layer, y, z, core, at], W.at[n.r], l_mv.at[n.r, 2]),
        )

    def c_a1(n):
        return copy(CL.at[n.k, 1 - y, row, near_part], A1.at[n.k], s_a1.at[n.s], r_a1.at[n.r], across)

    def c_a2(n, b, go_right):
        land, rs, ss, j, device = (AL, r_al, s_al, b - 1, right) if go_right else (AR, r_ar, s_ar, b, left)
        return copy(CL.at[n.k, y, at_z(b), near_part], land.at[n.k, j], ss.at[n.s, j], rs.at[n.r, j], device)

    def c_b1(n, b, go_right):
        land, rs, ss, j, device = (BL, r_bl, s_bl, b - 1, right) if go_right else (BR, r_br, s_br, b, left)
        return copy(CL.at[n.k, both, at_z(b), far_part], land.at[n.k, j], ss.at[n.s, j], rs.at[n.r, j], device)

    def c_b2(n):
        return copy(CL.at[n.k, 1 - y, at_z(z), far_part], B2.at[n.k], s_b2.at[n.s], r_b2.at[n.r], across)

    def same(n, rows, column, part, ss, rs, device):
        there = out.at[n.c, rows, column, plane, part]
        return copy(there, there, ss, rs, device)

    def c_yo(n):
        return same(n, y, z, whole, s_yo.at[n.s], r_yo.at[n.r], across)

    def c_az(n, b, go_right):
        ss, device = (s_azr, right) if go_right else (s_azl, left)
        return same(n, y, b, near_part, ss.at[n.s, b], r_az.at[n.r, b], device)

    def c_ay(n, b):
        return same(n, y, b, near_part, s_ay.at[n.s, b], r_ay.at[n.r, b], across)

    def c_bz(n, b, go_right):
        ss, device = (s_bzr, right) if go_right else (s_bzl, left)
        return same(n, both, b, far_part, ss.at[n.s, b], r_bz.at[n.r, b], device)

    def c_co(n, b):
        return same(n, both, b, whole, s_co.at[n.s, b], r_co.at[n.k], partner)

    def c_co_all(n):
        return same(n, both, row, whole, s_co.at[n.s, 0], r_co.at[n.k], partner)

    def start(copies):
        for one in copies if isinstance(copies, tuple) else (copies,):
            one.start()

    def sent(one):
        one.wait_send()

    def when(*conds):
        return pl.when(functools.reduce(jnp.logical_and, conds))

    def loop(low, high, body):
        lax.fori_loop(low, high, lambda i, _: (body(i), 0)[1], 0)

    def of_weight(n, do):
        for i in range(3):
            when(n.c >= 2 * i * pieces, n.c < 2 * (i + 1) * pieces)(functools.partial(do, i))

    def total(terms):
        return functools.reduce(jnp.add, (one.astype(F32) for one in terms))

    def a2(n, go_right, act, sums):
        def one(b):
            if sums:

                def put(inner):
                    spot = at_z(b)
                    terms = [G[n.g, y, spot, near_part], CL[n.k, y, spot, near_part], A1[n.k, spot]]
                    if inner:
                        terms.append(AL[n.k, b - 1] if go_right else AR[n.k, b])
                    CL[n.k, y, spot, near_part] = total(terms).astype(BF16)

                pl.when(z == (0 if go_right else 3))(lambda: put(False))
                pl.when(z != (0 if go_right else 3))(lambda: put(True))
            act(c_a2(n, b, go_right))

        loop(z + 1, 4, one) if go_right else loop(0, z, one)

    def b1(n, go_right, act, sums):
        def one(b):
            if sums:

                def put(inner):
                    spot = at_z(b)
                    terms = [G[n.g, both, spot, far_part], CL[n.k, both, spot, far_part]]
                    if inner:
                        terms.append(BL[n.k, b - 1] if go_right else BR[n.k, b])
                    CL[n.k, both, spot, far_part] = total(terms).astype(BF16)

                pl.when(z == (0 if go_right else 3))(lambda: put(False))
                pl.when(z != (0 if go_right else 3))(lambda: put(True))
            act(c_b1(n, b, go_right))

        loop(z + 1, 4, one) if go_right else loop(0, z, one)

    def arrived(n, go_right, make):
        if go_right:
            when(z > 0)(lambda: loop(z, 4, lambda b: make(n, b, True).wait_recv()))
        else:
            when(z < 3)(lambda: loop(0, z + 1, lambda b: make(n, b, False).wait_recv()))

    def own_part(n, yy, part, with_rows, land_l, land_r, extra, put):
        def terms():
            return [G[n.g, yy, at_z(z), part], CL[n.k, yy, at_z(z), part], *extra()]

        def from_left():
            return land_l[n.k, z - 1, yy] if with_rows else land_l[n.k, z - 1]

        def from_right():
            return land_r[n.k, z, yy] if with_rows else land_r[n.k, z]

        pl.when(z == 0)(lambda: put(total([*terms(), from_right()])))
        pl.when(z == 3)(lambda: put(total([*terms(), from_left()])))
        when(z > 0, z < 3)(lambda: put(total([*terms(), from_left(), from_right()])))

    def az(n, b, act):
        when(z < 3, b <= z)(lambda: act(c_az(n, b, True)))
        when(z > 0, b >= z)(lambda: act(c_az(n, b, False)))

    def bz(n, b, act):
        when(z < 3, b <= z)(lambda: act(c_bz(n, b, True)))
        when(z > 0, b >= z)(lambda: act(c_bz(n, b, False)))

    def sides(k):
        return ((z, z >= 0),) if k == 0 else ((z - k, z >= k), (z + k, z <= 3 - k))

    def step(t):
        tau = t - 2
        back = [Chunk(tau - k, N) for k in range(9 + LAG)]
        inward = {
            (late, kind, go_right): Chunk(tau - late - kind - (z if go_right else 3 - z), N)
            for late in (0, LAG)
            for kind in (0, 1)
            for go_right in (True, False)
        }
        first, ahead, last = Chunk(t, N), Chunk(t - 4, N), Chunk(tau - 9, N)

        @pl.when(first.ok)
        def _():
            of_weight(first, lambda i: (start(c_core(first, i)), start(c_g(first, i)), None)[2])

        @pl.when(ahead.ok)
        def _():
            of_weight(ahead, lambda i: start(c_load(ahead, i)))

        n0 = back[0]

        @pl.when(n0.ok)
        def _():
            c_g_all(n0).wait()
            c_core_all(n0).wait_recv()
            CL[n0.k, 1 - y, row, near_part] = total((G[n0.g, 1 - y, row, near_part], CL[n0.k, 1 - y, row, near_part])).astype(BF16)
            c_a1(n0).start()

        for go_right in (True, False):
            n = inward[0, 0, go_right]

            @pl.when(n.ok)
            def _():
                arrived(n, go_right, c_b1)
                b1(n, go_right, start, True)

        @pl.when(back[1].ok)
        def _():
            c_a1(back[1]).wait_recv()

        for go_right in (True, False):
            n = inward[0, 1, go_right]

            @pl.when(n.ok)
            def _():
                arrived(n, go_right, c_a2)
                a2(n, go_right, start, True)

        n3 = back[3]

        @pl.when(n3.ok)
        def _():
            def put(value):
                CL[n3.k, 1 - y, at_z(z), far_part] = value.astype(BF16)

            own_part(n3, 1 - y, far_part, True, BL, BR, lambda: (), put)
            c_b2(n3).start()

        n4 = back[4]

        @pl.when(n4.ok)
        def _():
            c_b2(n4).wait_recv()
            for one in c_load(n4, 0):
                one.wait()

            def put_near(value):
                GS[near_part] = value.astype(BF16)

            def put_far(value):
                GS[far_part] = value.astype(BF16)

            own_part(n4, y, near_part, False, AL, AR, lambda: (A1[n4.k, at_z(z)],), put_near)
            own_part(n4, y, far_part, True, BL, BR, lambda: (B2[n4.k],), put_far)
            g = GS[...].astype(F32)
            m = 0.9 * m_out[n4.c] + 0.1 * g
            v = 0.95 * v_out[n4.c] + 0.05 * g * g
            w = W[n4.r].astype(F32)
            out[n4.c, y, z, plane] = (w - 0.02 * (m * lax.rsqrt(v + 1e-8) + 0.1 * w)).astype(BF16)
            m_out[n4.c] = m
            v_out[n4.c] = v
            c_yo(n4).start()
            az(n4, z, start)

        for k in (1, 2, 3):
            n = back[4 + k]
            for b, there in sides(k):

                @when(n.ok, there)
                def _():
                    c_az(n, b, True).wait_recv()
                    az(n, b, start)
                    c_ay(n, b).start()

        for k in (0, 1, 2, 3):
            n = back[5 + k]
            for b, there in sides(k):

                @when(n.ok, there)
                def _():
                    if k == 0:
                        c_yo(n).wait_recv()
                    else:
                        c_bz(n, b, True).wait_recv()
                        c_ay(n, b).wait_recv()
                    bz(n, b, start)
                    c_co(n, b).start()

        @pl.when(last.ok)
        def _():
            c_co_all(last).wait_recv()

        @pl.when(back[LAG].ok)
        def _():
            sent(c_core_all(back[LAG]))
            sent(c_a1(back[LAG]))

        for go_right in (True, False):
            for kind, group in enumerate((b1, a2)):
                n = inward[LAG, kind, go_right]
                pl.when(n.ok)(functools.partial(group, n, go_right, sent, False))

        @pl.when(back[LAG + 3].ok)
        def _():
            sent(c_b2(back[LAG + 3]))

        @pl.when(back[LAG + 4].ok)
        def _():
            sent(c_yo(back[LAG + 4]))
            az(back[LAG + 4], z, sent)

        for k in (1, 2, 3):
            n = back[LAG + 4 + k]
            for b, there in sides(k):

                @when(n.ok, there)
                def _():
                    az(n, b, sent)
                    sent(c_ay(n, b))

        for k in (0, 1, 2, 3):
            n = back[LAG + 5 + k]
            for b, there in sides(k):

                @when(n.ok, there)
                def _():
                    bz(n, b, sent)
                    sent(c_co(n, b))

    loop(0, N + 2 + 8 + LAG, step)


def whole_step(pieces, near, arrays):
    tiles = arrays[6].shape[1]
    T, N = tiles // pieces, 6 * pieces
    TA, TB = near, T - near
    tile = (16, 128)
    dma = pltpu.SemaphoreType.DMA
    scratch = [
        pltpu.VMEM((RING, 2, 4, T, *tile), BF16),
        pltpu.VMEM((LAND, 2, 4, T, *tile), BF16),
        pltpu.VMEM((LAND, 4, TA, *tile), BF16),
        pltpu.VMEM((LAND, 3, TA, *tile), BF16),
        pltpu.VMEM((LAND, 3, TA, *tile), BF16),
        pltpu.VMEM((LAND, 3, 2, TB, *tile), BF16),
        pltpu.VMEM((LAND, 3, 2, TB, *tile), BF16),
        pltpu.VMEM((LAND, TB, *tile), BF16),
        pltpu.VMEM((ARRIVALS, T, *tile), BF16),
        pltpu.VMEM((T, *tile), BF16),
        dma((ARRIVALS,)), dma((ARRIVALS, 3)),
        dma((RING,)), dma((ARRIVALS,)), *(dma((ARRIVALS, 3)) for _ in range(4)), dma((ARRIVALS,)), dma((ARRIVALS,)),
        *(dma((ARRIVALS, 4)) for _ in range(3)), dma((LAND,)),
        dma((ARRIVALS,)), dma((SENDS,)), *(dma((SENDS, 3)) for _ in range(4)), dma((SENDS,)), dma((SENDS,)),
        *(dma((SENDS, 4)) for _ in range(6)),
    ]

    def body(*refs):
        kernel(pieces, tiles, near, refs[:12], refs[12:15], refs[15:])

    hbm, vmem = (pl.BlockSpec(memory_space=space) for space in (pl.ANY, pltpu.VMEM))
    return pl.pallas_call(
        body,
        out_shape=(
            pltpu.VMEM((N, T, *tile), F32),
            pltpu.VMEM((N, T, *tile), F32),
            pltpu.VMEM((N, 2, 4, 2, T, *tile), BF16),
        ),
        in_specs=[hbm] * 12,
        out_specs=(vmem,) * 3,
        scratch_shapes=scratch,
        compiler_params=pltpu.CompilerParams(collective_id=0, has_side_effects=True, vmem_limit_bytes=VMEM_LIMIT),
    )(*arrays)


def unload(m, v, w):
    N, T, *tile = m.shape
    pieces = N // 6

    def body(m, v, w, *refs):
        outs, sems = refs[:9], refs[9]
        for i in range(3):

            def one(c, _, i=i):
                layer = lax.div(c, pieces)
                for y, z in itertools.product(range(2), range(4)):
                    for plane in range(2):
                        there = outs[i].at[layer, y, z, (plane + y + z) % 2, c - layer * pieces]
                        pltpu.make_async_copy(w.at[2 * i * pieces + c, y, z, plane], there, sems.at[i]).start()
                return 0

            lax.fori_loop(0, 2 * pieces, one, 0)
            here = pl.ds(2 * i * pieces, 2 * pieces)
            pltpu.make_async_copy(m.at[here], outs[3 + i], sems.at[3 + i]).start()
            pltpu.make_async_copy(v.at[here], outs[6 + i], sems.at[6 + i]).start()
        for i in range(9):
            pltpu.make_async_copy(outs[i], outs[i], sems.at[i]).wait()

    given = [pltpu.with_memory_space_constraint(a, pltpu.VMEM) for a in (m, v, w)]
    return pl.pallas_call(
        body,
        out_shape=(jax.ShapeDtypeStruct((2, 2, 4, 2, pieces, T, *tile), BF16),) * 3
        + (jax.ShapeDtypeStruct((2 * pieces, T, *tile), F32),) * 6,
        in_specs=[pl.BlockSpec(memory_space=pltpu.VMEM)] * 3,
        out_specs=(pl.BlockSpec(memory_space=pl.ANY),) * 9,
        scratch_shapes=[pltpu.SemaphoreType.DMA((9,))],
        compiler_params=pltpu.CompilerParams(vmem_limit_bytes=1 << 20),
    )(*given)


def to_tiles(a):
    _, r, c = a.shape
    return a.reshape(2, r // 8, 8, c // 128, 128).swapaxes(2, 3).reshape(2, -1, 16, 128)


def from_tiles(a, shape):
    _, r, c = shape
    return a.reshape(2, r // 8, c // 128, 8, 128).swapaxes(2, 3).reshape(shape)


def solution(mesh):
    def step(*arrays):
        arrays = [a.reshape(a.shape[-3:]) for a in arrays]
        tiled = [to_tiles(a) for a in arrays]
        blocks = tiled[6].shape[1]
        tiled = [t.reshape(2, 2, 2, 2, 2, blocks, 16, 128) for t in tiled[:3]] + [t.reshape(2, 2, 4, 2, blocks, 16, 128) for t in tiled[3:6]] + tiled[6:]
        results = unload(*whole_step(PIECES, 6 * blocks // (10 * PIECES), tiled))
        shapes = [a.shape for a in arrays[3:9]] + [a.shape for a in arrays[6:9]]
        return tuple(from_tiles(one, shape) for one, shape in zip(results, shapes, strict=True))

    all_of, cut = P(None, None, None), P(None, "dp", None)
    return jax.shard_map(
        step,
        mesh=mesh,
        in_specs=(P(("rep", "dp"), None, None, None),) * 3 + (all_of,) * 3 + (cut,) * 6,
        out_specs=(P("rep", None, None),) * 3 + (P("rep", "dp", None),) * 6,
        check_vma=False,
    )
```

```python
import functools
import itertools

import jax
import jax.numpy as jnp
from jax import lax
from jax.experimental import pallas as pl
from jax.experimental.pallas import tpu as pltpu
from jax.sharding import PartitionSpec as P

PIECES = 10
LAND = 16
RING = 8
LAG = 1
SENDS = 2
ARRIVALS = 4
VMEM_LIMIT = 15 << 20
F32, BF16 = jnp.float32, jnp.bfloat16


class Chunk:
    def __init__(self, c, count):
        self.c = c
        self.ok = jnp.logical_and(c >= 0, c < count)
        self.s, self.r, self.g, self.k = (lax.rem(c + 64, n) for n in (SENDS, ARRIVALS, RING, LAND))


def kernel(pieces, tiles, near, refs_in, refs_out, scratch):
    g_in, w_in, m_in, v_in = (refs_in[i : i + 3] for i in (0, 3, 6, 9))
    m_out, v_out, out = refs_out
    (G, CL, A1, AL, AR, BL, BR, B2, W, GS) = scratch[:10]
    (l_g, l_mv) = scratch[10:12]
    (r_core, r_a1, r_al, r_ar, r_bl, r_br, r_b2, r_yo, r_az, r_ay, r_bz, r_co) = scratch[12:24]
    (s_core, s_a1, s_al, s_ar, s_bl, s_br, s_b2, s_yo, s_azr, s_azl, s_ay, s_bzr, s_bzl, s_co) = scratch[24:]
    T = tiles // pieces
    TA, TB = near, T - near
    N = 6 * pieces
    x, me = lax.axis_index("rep"), lax.axis_index("dp")
    core, z, y = me % 2, (me // 2) % 4, me // 8
    plane, other = (core + y + z) % 2, 1 - 2 * core
    partner, right, left, across = me + other, me + 2 + other, me - 2 + other, me + 8 - 16 * y + other

    barrier = pltpu.get_barrier_semaphore()

    def greet(device):
        pl.semaphore_signal(barrier, inc=1, device_id=(x, device), device_id_type=pl.DeviceIdType.MESH)

    greet(partner)
    greet(across)

    @pl.when(z > 0)
    def _():
        greet(left)

    @pl.when(z < 3)
    def _():
        greet(right)

    pl.semaphore_wait(barrier, 2 + jnp.where(z > 0, 1, 0) + jnp.where(z < 3, 1, 0))

    def copy(src, dst, ss, rs, device):
        return pltpu.make_async_remote_copy(
            src_ref=src, dst_ref=dst, send_sem=ss, recv_sem=rs, device_id=(x, device), device_id_type=pl.DeviceIdType.MESH
        )

    both, row, near_part, far_part, whole = pl.ds(0, 2), pl.ds(0, 4), pl.ds(0, TA), pl.ds(TA, TB), pl.ds(0, T)

    def place(c):
        layers = lax.div(c, pieces)
        return lax.rem(layers, 2), pl.ds((c - layers * pieces) * T, T)

    def at_z(b):
        return 2 * lax.rem(b, 2) + lax.div(b, 2)

    def terms_of(n, i, which, slot):
        layer, at = place(n.c)
        for yy in range(2):
            for odd in range(2):
                its = which if yy == odd else 1 - which
                yield g_in[i].at[layer, yy, both, odd, its, at], slot.at[yy, pl.ds(2 * odd, 2)]

    def c_core(n, i):
        return tuple(copy(src, dst, s_core.at[n.r], r_core.at[n.g], partner) for src, dst in terms_of(n, i, 1 - plane, CL.at[n.k]))

    def c_core_all(n):
        return copy(CL.at[n.k], CL.at[n.k], s_core.at[n.r], r_core.at[n.g], partner)

    def c_g(n, i):
        return tuple(pltpu.make_async_copy(src, dst, l_g.at[n.r]) for src, dst in terms_of(n, i, plane, G.at[n.g]))

    def c_g_all(n):
        return pltpu.make_async_copy(G.at[n.g], G.at[n.g], l_g.at[n.r])

    def c_load(n, i):
        layer, at = place(n.c)
        return (
            pltpu.make_async_copy(m_in[i].at[layer, at], m_out.at[n.c], l_mv.at[n.r, 0]),
            pltpu.make_async_copy(v_in[i].at[layer, at], v_out.at[n.c], l_mv.at[n.r, 1]),
            pltpu.make_async_copy(w_in[i].at[layer, y, z, core, at], W.at[n.r], l_mv.at[n.r, 2]),
        )

    def c_a1(n):
        return copy(CL.at[n.k, 1 - y, row, near_part], A1.at[n.k], s_a1.at[n.s], r_a1.at[n.r], across)

    def c_a2(n, b, go_right):
        land, rs, ss, j, device = (AL, r_al, s_al, b - 1, right) if go_right else (AR, r_ar, s_ar, b, left)
        return copy(CL.at[n.k, y, at_z(b), near_part], land.at[n.k, j], ss.at[n.s, j], rs.at[n.r, j], device)

    def c_b1(n, b, go_right):
        land, rs, ss, j, device = (BL, r_bl, s_bl, b - 1, right) if go_right else (BR, r_br, s_br, b, left)
        return copy(CL.at[n.k, both, at_z(b), far_part], land.at[n.k, j], ss.at[n.s, j], rs.at[n.r, j], device)

    def c_b2(n):
        return copy(CL.at[n.k, 1 - y, at_z(z), far_part], B2.at[n.k], s_b2.at[n.s], r_b2.at[n.r], across)

    def same(n, rows, column, part, ss, rs, device):
        there = out.at[n.c, rows, column, plane, part]
        return copy(there, there, ss, rs, device)

    def c_yo(n):
        return same(n, y, z, whole, s_yo.at[n.s], r_yo.at[n.r], across)

    def c_az(n, b, go_right):
        ss, device = (s_azr, right) if go_right else (s_azl, left)
        return same(n, y, b, near_part, ss.at[n.s, b], r_az.at[n.r, b], device)

    def c_ay(n, b):
        return same(n, y, b, near_part, s_ay.at[n.s, b], r_ay.at[n.r, b], across)

    def c_bz(n, b, go_right):
        ss, device = (s_bzr, right) if go_right else (s_bzl, left)
        return same(n, both, b, far_part, ss.at[n.s, b], r_bz.at[n.r, b], device)

    def c_co(n, b):
        return same(n, both, b, whole, s_co.at[n.s, b], r_co.at[n.k], partner)

    def c_co_all(n):
        return same(n, both, row, whole, s_co.at[n.s, 0], r_co.at[n.k], partner)

    def start(copies):
        for one in copies if isinstance(copies, tuple) else (copies,):
            one.start()

    def sent(one):
        one.wait_send()

    def when(*conds):
        return pl.when(functools.reduce(jnp.logical_and, conds))

    def loop(low, high, body):
        lax.fori_loop(low, high, lambda i, _: (body(i), 0)[1], 0)

    def of_weight(n, do):
        for i in range(3):
            when(n.c >= 2 * i * pieces, n.c < 2 * (i + 1) * pieces)(functools.partial(do, i))

    def total(terms):
        return functools.reduce(jnp.add, (one.astype(F32) for one in terms))

    def a2(n, go_right, act, sums):
        def one(b):
            if sums:

                def put(inner):
                    spot = at_z(b)
                    terms = [G[n.g, y, spot, near_part], CL[n.k, y, spot, near_part], A1[n.k, spot]]
                    if inner:
                        terms.append(AL[n.k, b - 1] if go_right else AR[n.k, b])
                    CL[n.k, y, spot, near_part] = total(terms).astype(BF16)

                pl.when(z == (0 if go_right else 3))(lambda: put(False))
                pl.when(z != (0 if go_right else 3))(lambda: put(True))
            act(c_a2(n, b, go_right))

        loop(z + 1, 4, one) if go_right else loop(0, z, one)

    def b1(n, go_right, act, sums):
        def one(b):
            if sums:

                def put(inner):
                    spot = at_z(b)
                    terms = [G[n.g, both, spot, far_part], CL[n.k, both, spot, far_part]]
                    if inner:
                        terms.append(BL[n.k, b - 1] if go_right else BR[n.k, b])
                    CL[n.k, both, spot, far_part] = total(terms).astype(BF16)

                pl.when(z == (0 if go_right else 3))(lambda: put(False))
                pl.when(z != (0 if go_right else 3))(lambda: put(True))
            act(c_b1(n, b, go_right))

        loop(z + 1, 4, one) if go_right else loop(0, z, one)

    def arrived(n, go_right, make):
        if go_right:
            when(z > 0)(lambda: loop(z, 4, lambda b: make(n, b, True).wait_recv()))
        else:
            when(z < 3)(lambda: loop(0, z + 1, lambda b: make(n, b, False).wait_recv()))

    def own_part(n, yy, part, with_rows, land_l, land_r, extra, put):
        def terms():
            return [G[n.g, yy, at_z(z), part], CL[n.k, yy, at_z(z), part], *extra()]

        def from_left():
            return land_l[n.k, z - 1, yy] if with_rows else land_l[n.k, z - 1]

        def from_right():
            return land_r[n.k, z, yy] if with_rows else land_r[n.k, z]

        pl.when(z == 0)(lambda: put(total([*terms(), from_right()])))
        pl.when(z == 3)(lambda: put(total([*terms(), from_left()])))
        when(z > 0, z < 3)(lambda: put(total([*terms(), from_left(), from_right()])))

    def az(n, b, act):
        when(z < 3, b <= z)(lambda: act(c_az(n, b, True)))
        when(z > 0, b >= z)(lambda: act(c_az(n, b, False)))

    def bz(n, b, act):
        when(z < 3, b <= z)(lambda: act(c_bz(n, b, True)))
        when(z > 0, b >= z)(lambda: act(c_bz(n, b, False)))

    def sides(k):
        return ((z, z >= 0),) if k == 0 else ((z - k, z >= k), (z + k, z <= 3 - k))

    def step(t):
        tau = t - 2
        back = [Chunk(tau - k, N) for k in range(9 + LAG)]
        inward = {
            (late, kind, go_right): Chunk(tau - late - kind - (z if go_right else 3 - z), N)
            for late in (0, LAG)
            for kind in (0, 1)
            for go_right in (True, False)
        }
        first, ahead, last = Chunk(t, N), Chunk(t - 4, N), Chunk(tau - 9, N)

        @pl.when(first.ok)
        def _():
            of_weight(first, lambda i: (start(c_core(first, i)), start(c_g(first, i)), None)[2])

        @pl.when(ahead.ok)
        def _():
            of_weight(ahead, lambda i: start(c_load(ahead, i)))

        n0 = back[0]

        @pl.when(n0.ok)
        def _():
            c_g_all(n0).wait()
            c_core_all(n0).wait_recv()
            CL[n0.k, 1 - y, row, near_part] = total((G[n0.g, 1 - y, row, near_part], CL[n0.k, 1 - y, row, near_part])).astype(BF16)
            c_a1(n0).start()

        for go_right in (True, False):
            n = inward[0, 0, go_right]

            @pl.when(n.ok)
            def _():
                arrived(n, go_right, c_b1)
                b1(n, go_right, start, True)

        @pl.when(back[1].ok)
        def _():
            c_a1(back[1]).wait_recv()

        for go_right in (True, False):
            n = inward[0, 1, go_right]

            @pl.when(n.ok)
            def _():
                arrived(n, go_right, c_a2)
                a2(n, go_right, start, True)

        n3 = back[3]

        @pl.when(n3.ok)
        def _():
            def put(value):
                CL[n3.k, 1 - y, at_z(z), far_part] = value.astype(BF16)

            own_part(n3, 1 - y, far_part, True, BL, BR, lambda: (), put)
            c_b2(n3).start()

        n4 = back[4]

        @pl.when(n4.ok)
        def _():
            c_b2(n4).wait_recv()
            for one in c_load(n4, 0):
                one.wait()

            def put_near(value):
                GS[near_part] = value.astype(BF16)

            def put_far(value):
                GS[far_part] = value.astype(BF16)

            own_part(n4, y, near_part, False, AL, AR, lambda: (A1[n4.k, at_z(z)],), put_near)
            own_part(n4, y, far_part, True, BL, BR, lambda: (B2[n4.k],), put_far)
            g = GS[...].astype(F32)
            m = 0.9 * m_out[n4.c] + 0.1 * g
            v = 0.95 * v_out[n4.c] + 0.05 * g * g
            w = W[n4.r].astype(F32)
            out[n4.c, y, z, plane] = (w - 0.02 * (m * lax.rsqrt(v + 1e-8) + 0.1 * w)).astype(BF16)
            m_out[n4.c] = m
            v_out[n4.c] = v
            c_yo(n4).start()
            az(n4, z, start)

        for k in (1, 2, 3):
            n = back[4 + k]
            for b, there in sides(k):

                @when(n.ok, there)
                def _():
                    c_az(n, b, True).wait_recv()
                    az(n, b, start)
                    c_ay(n, b).start()

        for k in (0, 1, 2, 3):
            n = back[5 + k]
            for b, there in sides(k):

                @when(n.ok, there)
                def _():
                    if k == 0:
                        c_yo(n).wait_recv()
                    else:
                        c_bz(n, b, True).wait_recv()
                        c_ay(n, b).wait_recv()
                    bz(n, b, start)
                    c_co(n, b).start()

        @pl.when(last.ok)
        def _():
            c_co_all(last).wait_recv()

        @pl.when(back[LAG].ok)
        def _():
            sent(c_core_all(back[LAG]))
            sent(c_a1(back[LAG]))

        for go_right in (True, False):
            for kind, group in enumerate((b1, a2)):
                n = inward[LAG, kind, go_right]
                pl.when(n.ok)(functools.partial(group, n, go_right, sent, False))

        @pl.when(back[LAG + 3].ok)
        def _():
            sent(c_b2(back[LAG + 3]))

        @pl.when(back[LAG + 4].ok)
        def _():
            sent(c_yo(back[LAG + 4]))
            az(back[LAG + 4], z, sent)

        for k in (1, 2, 3):
            n = back[LAG + 4 + k]
            for b, there in sides(k):

                @when(n.ok, there)
                def _():
                    az(n, b, sent)
                    sent(c_ay(n, b))

        for k in (0, 1, 2, 3):
            n = back[LAG + 5 + k]
            for b, there in sides(k):

                @when(n.ok, there)
                def _():
                    bz(n, b, sent)
                    sent(c_co(n, b))

    loop(0, N + 2 + 8 + LAG, step)


def whole_step(pieces, near, arrays):
    tiles = arrays[6].shape[1]
    T, N = tiles // pieces, 6 * pieces
    TA, TB = near, T - near
    tile = (16, 128)
    dma = pltpu.SemaphoreType.DMA
    scratch = [
        pltpu.VMEM((RING, 2, 4, T, *tile), BF16),
        pltpu.VMEM((LAND, 2, 4, T, *tile), BF16),
        pltpu.VMEM((LAND, 4, TA, *tile), BF16),
        pltpu.VMEM((LAND, 3, TA, *tile), BF16),
        pltpu.VMEM((LAND, 3, TA, *tile), BF16),
        pltpu.VMEM((LAND, 3, 2, TB, *tile), BF16),
        pltpu.VMEM((LAND, 3, 2, TB, *tile), BF16),
        pltpu.VMEM((LAND, TB, *tile), BF16),
        pltpu.VMEM((ARRIVALS, T, *tile), BF16),
        pltpu.VMEM((T, *tile), BF16),
        dma((ARRIVALS,)), dma((ARRIVALS, 3)),
        dma((RING,)), dma((ARRIVALS,)), *(dma((ARRIVALS, 3)) for _ in range(4)), dma((ARRIVALS,)), dma((ARRIVALS,)),
        *(dma((ARRIVALS, 4)) for _ in range(3)), dma((LAND,)),
        dma((ARRIVALS,)), dma((SENDS,)), *(dma((SENDS, 3)) for _ in range(4)), dma((SENDS,)), dma((SENDS,)),
        *(dma((SENDS, 4)) for _ in range(6)),
    ]

    def body(*refs):
        kernel(pieces, tiles, near, refs[:12], refs[12:15], refs[15:])

    hbm, vmem = (pl.BlockSpec(memory_space=space) for space in (pl.ANY, pltpu.VMEM))
    return pl.pallas_call(
        body,
        out_shape=(
            pltpu.VMEM((N, T, *tile), F32),
            pltpu.VMEM((N, T, *tile), F32),
            pltpu.VMEM((N, 2, 4, 2, T, *tile), BF16),
        ),
        in_specs=[hbm] * 12,
        out_specs=(vmem,) * 3,
        scratch_shapes=scratch,
        compiler_params=pltpu.CompilerParams(collective_id=0, has_side_effects=True, vmem_limit_bytes=VMEM_LIMIT),
    )(*arrays)


def unload(m, v, w):
    N, T, *tile = m.shape
    pieces = N // 6

    def body(m, v, w, *refs):
        outs, sems = refs[:9], refs[9]
        for i in range(3):

            def one(c, _, i=i):
                layer = lax.div(c, pieces)
                for y, z in itertools.product(range(2), range(4)):
                    for plane in range(2):
                        for part in (pl.ds(0, T // 2), pl.ds(T // 2, T - T // 2)):
                            there = outs[i].at[layer, y, z, (plane + y + z) % 2, c - layer * pieces, part]
                            pltpu.make_async_copy(w.at[2 * i * pieces + c, y, z, plane, part], there, sems.at[i]).start()
                for given, j in ((m, 3 + i), (v, 6 + i)):
                    pltpu.make_async_copy(given.at[2 * i * pieces + c], outs[j].at[c], sems.at[j]).start()
                return 0

            lax.fori_loop(0, 2 * pieces, one, 0)
        for i in range(9):
            pltpu.make_async_copy(outs[i], outs[i], sems.at[i]).wait()

    given = [pltpu.with_memory_space_constraint(a, pltpu.VMEM) for a in (m, v, w)]
    return pl.pallas_call(
        body,
        out_shape=(jax.ShapeDtypeStruct((2, 2, 4, 2, pieces, T, *tile), BF16),) * 3
        + (jax.ShapeDtypeStruct((2 * pieces, T, *tile), F32),) * 6,
        in_specs=[pl.BlockSpec(memory_space=pltpu.VMEM)] * 3,
        out_specs=(pl.BlockSpec(memory_space=pl.ANY),) * 9,
        scratch_shapes=[pltpu.SemaphoreType.DMA((9,))],
        compiler_params=pltpu.CompilerParams(vmem_limit_bytes=1 << 20),
    )(*given)


def to_tiles(a):
    _, r, c = a.shape
    return a.reshape(2, r // 8, 8, c // 128, 128).swapaxes(2, 3).reshape(2, -1, 16, 128)


def from_tiles(a, shape):
    _, r, c = shape
    return a.reshape(2, r // 8, c // 128, 8, 128).swapaxes(2, 3).reshape(shape)


def solution(mesh):
    def step(*arrays):
        arrays = [a.reshape(a.shape[-3:]) for a in arrays]
        tiled = [to_tiles(a) for a in arrays]
        blocks = tiled[6].shape[1]
        tiled = [t.reshape(2, 2, 2, 2, 2, blocks, 16, 128) for t in tiled[:3]] + [t.reshape(2, 2, 4, 2, blocks, 16, 128) for t in tiled[3:6]] + tiled[6:]
        results = unload(*whole_step(PIECES, 6 * blocks // (10 * PIECES), tiled))
        shapes = [a.shape for a in arrays[3:9]] + [a.shape for a in arrays[6:9]]
        return tuple(from_tiles(one, shape) for one, shape in zip(results, shapes, strict=True))

    all_of, cut = P(None, None, None), P(None, "dp", None)
    return jax.shard_map(
        step,
        mesh=mesh,
        in_specs=(P(("rep", "dp"), None, None, None),) * 3 + (all_of,) * 3 + (cut,) * 6,
        out_specs=(P("rep", None, None),) * 3 + (P("rep", "dp", None),) * 6,
        check_vma=False,
    )
```
